128 devices in a mesh: gx: 4 (over z_hi, core), gy: 4 (over y), gz: 8 (over z_lo, x).
Axes of the slice: x: 4, y: 4, z: 4 (z_hi: 2, z_lo: 2; z = z_hi * 2 + z_lo), core: 2. Of those that a mesh axis runs over, the one named last changes fastest.
Arguments:
- grads: bfloat16 [8, 2048, 3584], P('gz', ('gx', 'gy')), may hold values from -300 to 300
- momentum: float32 [2048, 3584], P(('gx', 'gy')), may hold values from -0.8 to 0.8
- variance: float32 [2048, 3584], P(('gx', 'gy'), 'gz'), may hold values from 0.25 to 4
- master: float32 [2048, 3584], P(('gx', 'gy', 'gz')), may hold values from -6 to 6
Outputs:
- weights: bfloat16 [2048, 3584], replicated
- new_master: float32 [2048, 3584], P(('gx', 'gy', 'gz'))
- new_momentum: float32 [2048, 3584], P(('gx', 'gy', 'gz'))
- worker_error: float32 [8, 2048, 3584], P('gz', ('gx', 'gy'))
The draws below stay inside these ranges and needn't reach their ends.
All inputs are finite; a program needn't handle non-finite values.
Results may differ from the reference program's by a relative error of at most 0.007.
Values may be sent and summed in bfloat16 or wider, within the bound.
A program may use at most 128 MiB of HBM per device.

```python
import math
import jax
import jax.numpy as jnp
from jax import lax

D = 3584
ROWS = 2048
WORKERS = 8


def joint_draw(key):
    base = jax.random.fold_in(key, 11)
    streams = jax.random.split(base, 5)
    momentum = jnp.clip(0.2 * jax.random.normal(streams[0], (ROWS, D), jnp.float32), -0.8, 0.8)
    magnitude = jnp.exp(jax.random.uniform(streams[2], (WORKERS, ROWS, D), jnp.float32, math.log(0.3), 0.0))
    positive = jax.random.bernoulli(streams[1], 0.5, (WORKERS, ROWS, D))
    signs = jnp.where(positive, 1.0, -1.0).astype(jnp.float32)
    row_scale = jnp.exp(jax.random.uniform(streams[3], (WORKERS, ROWS, 1), jnp.float32, math.log(0.3), math.log(3.0)))
    col_scale = jnp.exp(jax.random.uniform(streams[4], (1, 1, D), jnp.float32, math.log(0.3), math.log(3.0)))
    growth = 1.0 + 2.0 * jnp.arange(WORKERS, dtype=jnp.float32) / max(WORKERS - 1, 1)
    corrected = signs * magnitude * row_scale * col_scale * growth[:, None, None]
    grads = (corrected - 0.9 * momentum[None]) / 0.1
    return (grads, momentum)


def draw_grads(key, part):
    grads, momentum = joint_draw(key)
    return grads.astype(jnp.bfloat16)


def draw_momentum(key, part):
    grads, momentum = joint_draw(key)
    return momentum


def block_scale(key, extent, shards, least, largest):
    def one(dim, blocks):
        heights = jax.random.uniform(jax.random.fold_in(jax.random.fold_in(key, 6), dim), (blocks,), jnp.float32, least / len(shards), largest / len(shards))
        return jnp.repeat(jnp.exp(heights), extent[dim] // blocks).reshape((-1,) + (1,) * (len(extent) - dim - 1))

    factor_of = one(*shards[0])
    for cut in shards[1:]:
        factor_of = factor_of * one(*cut)
    return factor_of


def bell_draw(rng, extent, deviation, bound, cuts=(), kind=jnp.bfloat16):
    factor_of = block_scale(rng, extent, cuts, -0.22, 0.18) if cuts else 1.0
    array = jax.random.normal(rng, extent, jnp.float32) * deviation * factor_of
    return jnp.minimum(jnp.maximum(array, -bound), bound).astype(kind)


def setup_inputs(seed: int = 0) -> dict:
    key_list = jax.random.split(jax.random.key(seed), 5)
    return {
        "grads": draw_grads(jax.random.fold_in(key_list[4], 71), 0),
        "momentum": draw_momentum(jax.random.fold_in(key_list[4], 71), 0),
        "variance": jnp.clip(jnp.exp(math.log(4.0) - 2.7725887 * jax.random.uniform(key_list[2], (ROWS, D), jnp.float32) ** block_scale(key_list[2], (ROWS, D), ((0, 16), (1, 8)), -0.2, 0.2)), 0.25, 4.0),
        "master": bell_draw(key_list[3], (ROWS, D), 1.0, 6.0, ((0, 128),), jnp.float32),
    }


beta_one = 0.9
learning_rate = 0.25
epsilon = 1e-08

def reference(grads, momentum, variance, master):
    corrected = beta_one * momentum[None] + (1.0 - beta_one) * grads.astype(jnp.float32)
    level = lax.optimization_barrier(jnp.mean(jnp.abs(corrected), axis=-1, keepdims=True)).astype(jnp.bfloat16)
    signs = jnp.where(corrected >= 0.0, 1.0, -1.0).astype(jnp.float32)
    compressed = (level.astype(jnp.float32) * signs).astype(jnp.bfloat16)
    worker_error = corrected - compressed.astype(jnp.float32)
    new_momentum = lax.optimization_barrier(jnp.sum(compressed.astype(jnp.float32), axis=0)) / WORKERS
    new_master = master - learning_rate * new_momentum / (jnp.sqrt(variance) + epsilon)
    weights = new_master.astype(jnp.bfloat16)
    return (weights, new_master, new_momentum, worker_error)
```

```python
import jax
import jax.numpy as jnp
from jax import lax
from jax.experimental import pallas as pl
from jax.experimental.pallas import tpu as pltpu
from jax.sharding import PartitionSpec as P

beta_one = 0.9
learning_rate = 0.25
epsilon = 1e-08

MESH = pl.DeviceIdType.MESH
WORKERS = 8
ROWS = 16
WIDTH = 3584
PIECE = WIDTH // WORKERS
BLOCKS = 128

COLUMNS = ((0, 1280), (1280, 1152), (2432, 1152))
DIMS = (("x", "y", "z"), ("y", "z", "x"), ("z", "x", "y"))


def block_index(p):
    return (((p["z"] // 2) * 2 + p["c"]) * 4 + p["y"]) * 8 + (p["z"] % 2) * 4 + p["x"]


def device(p):
    return ((p["z"] // 2) * 2 + p["c"], p["y"], (p["z"] % 2) * 4 + p["x"])


def moved(p, dim, by):
    q = dict(p)
    q[dim] = lax.rem(p[dim] + by + 4, 4)
    return q


def line(w, p, color, half=None):
    start, size = COLUMNS[color]
    cols = pl.ds(start, size)
    first = DIMS[color][0]
    part = slice(None) if half is None else pl.ds(half * 2, 2)
    zh, zl = p["z"] // 2, p["z"] % 2
    if first == "x":
        return w.at[zh, p["c"], p["y"], zl, part, :, cols]
    if first == "y":
        return w.at[zh, p["c"], part, zl, p["x"], :, cols]
    if half is None:
        return w.at[:, p["c"], p["y"], :, p["x"], :, cols]
    return w.at[half, p["c"], p["y"], :, p["x"], :, cols]


def unit(w, p, color):
    start, size = COLUMNS[color]
    return w.at[p["z"] // 2, p["c"], p["y"], p["z"] % 2, p["x"], :, pl.ds(start, size)]


def step_kernel(
    g_ref, m_ref, v_ref, master_ref,
    w, new_master_ref, new_momentum_ref, error_ref,
    sent, received, var_sent, var_received,
    send_sem, exchange_sem, var_sem, gather_sem, relay_sem, relay_send_sem, var_send_sem, exchange_send_sem,
):
    gx, gy, gz = lax.axis_index("gx"), lax.axis_index("gy"), lax.axis_index("gz")
    me = {"x": lax.rem(gz, 4), "y": gy, "z": (gx // 2) * 2 + gz // 4, "c": lax.rem(gx, 2)}
    partner = dict(me, c=1 - me["c"])

    barrier = pltpu.get_barrier_semaphore()
    greeted = [(gx, gy, lax.rem(gz + k, WORKERS)) for k in range(1, WORKERS)]
    greeted += [device(moved(me, "y", k)) for k in (1, 2, 3)]
    greeted += [device(moved(me, "z", k)) for k in (1, 2, 3)]
    greeted += [device(partner)]

    for d in greeted:
        pl.semaphore_signal(barrier, inc=1, device_id=d, device_id_type=MESH)

    var = v_ref[...].T.astype(jnp.bfloat16)
    for k in range(WORKERS):
        var_sent[k] = var[k * ROWS:(k + 1) * ROWS, :]

    def compress(owner):
        rows = pl.ds(pl.multiple_of(owner * ROWS, ROWS), ROWS)
        corrected = beta_one * m_ref[rows, :] + (1.0 - beta_one) * g_ref[0, rows, :].astype(jnp.float32)
        level = jnp.mean(jnp.abs(corrected), axis=-1, keepdims=True).astype(jnp.bfloat16).astype(jnp.float32)
        compressed = jnp.where(corrected >= 0.0, level, -level)
        sent[owner] = compressed.astype(jnp.bfloat16)
        error_ref[rows, :] = corrected - compressed

    def exchange(k):
        owner = lax.rem(gz + k, WORKERS)
        return pltpu.make_async_remote_copy(
            src_ref=sent.at[owner], dst_ref=received.at[gz],
            send_sem=exchange_send_sem.at[k], recv_sem=exchange_sem.at[WORKERS - k],
            device_id=(gx, gy, owner), device_id_type=MESH)

    def var_exchange(k):
        owner = lax.rem(gz + k, WORKERS)
        return pltpu.make_async_remote_copy(
            src_ref=var_sent.at[owner], dst_ref=var_received.at[gz],
            send_sem=var_send_sem.at[k], recv_sem=var_sem.at[WORKERS - k],
            device_id=(gx, gy, owner), device_id_type=MESH)

    def exchange_in(k):
        source = lax.rem(gz + k, WORKERS)
        return pltpu.make_async_remote_copy(
            src_ref=sent.at[source], dst_ref=received.at[source],
            send_sem=exchange_send_sem.at[k], recv_sem=exchange_sem.at[k],
            device_id=(gx, gy, source), device_id_type=MESH)

    def var_exchange_in(k):
        source = lax.rem(gz + k, WORKERS)
        return pltpu.make_async_remote_copy(
            src_ref=var_sent.at[source], dst_ref=var_received.at[source],
            send_sem=var_send_sem.at[k], recv_sem=var_sem.at[k],
            device_id=(gx, gy, source), device_id_type=MESH)

    compress(lax.rem(gz + 1, WORKERS))
    pl.semaphore_wait(barrier, len(greeted))

    @pl.loop(1, WORKERS)
    def _(k):
        compress(lax.rem(gz + k + 1, WORKERS))
        exchange(k).start()
        var_exchange(k).start()

    received[gz] = sent[gz]
    var_received[gz] = var_sent[gz]

    @pl.loop(1, WORKERS)
    def _(k):
        exchange_in(k).wait_recv()
        var_exchange_in(k).wait_recv()

    mine = block_index(me)
    for pair in range(WORKERS // 2):
        cols = pl.ds(pair * 2 * PIECE, 2 * PIECE)
        total = received[0, :, cols].astype(jnp.float32)
        for k in range(1, WORKERS):
            total = total + received[k, :, cols].astype(jnp.float32)
        new_momentum = total / WORKERS
        owned = jnp.concatenate(
            [var_received[2 * pair].astype(jnp.float32), var_received[2 * pair + 1].astype(jnp.float32)], axis=-1)
        new_master = master_ref[:, cols] - learning_rate * new_momentum / (jnp.sqrt(owned) + epsilon)
        new_momentum_ref[:, cols] = new_momentum
        new_master_ref[:, cols] = new_master
        w[me["z"] // 2, me["c"], me["y"], me["z"] % 2, me["x"], :, cols] = new_master.astype(jnp.bfloat16)

    def put(src, to, sem):
        pltpu.make_async_remote_copy(
            src_ref=src, dst_ref=src, send_sem=send_sem, recv_sem=sem, device_id=device(to), device_id_type=MESH).start()

    def arrived(dst, sem):
        pltpu.make_async_remote_copy(
            src_ref=dst, dst_ref=dst, send_sem=send_sem, recv_sem=sem, device_id=device(partner), device_id_type=MESH).wait_recv()

    def relay(src):
        pltpu.make_async_remote_copy(
            src_ref=src, dst_ref=src, send_sem=relay_send_sem, recv_sem=relay_sem,
            device_id=device(partner), device_id_type=MESH).start()

    colors = range(3)

    for c in colors:
        for by in (1, 3, 2):
            put(unit(w, me, c), moved(me, DIMS[c][0], by), gather_sem.at[c, by - 1])

    for c in colors:
        for by in (1, 3, 2):
            arrived(unit(w, moved(me, DIMS[c][0], -by), c), gather_sem.at[c, by - 1])

    def spread(c, dim, src, at):
        put(src, moved(me, dim, 1), gather_sem.at[c, at])
        put(src, moved(me, dim, 3), gather_sem.at[c, at + 1])

    def onward(c, dim, p, direction, at):
        half = 0 if direction == 1 else 1
        put(line(w, p, c, half), moved(me, dim, direction), gather_sem.at[c, at + 2 + half])

    def source(dim, by, p=me):
        return moved(p, dim, -by)

    SECOND = 3
    THIRD = (7, 11, 15, 19)
    BY = (0, 1, 3, 2)

    for c in colors:
        spread(c, DIMS[c][1], line(w, me, c), SECOND)
    for c in colors:
        spread(c, DIMS[c][2], line(w, me, c), THIRD[0])
        relay(line(w, me, c))

    def third(c, i):
        p = source(DIMS[c][1], BY[i])
        spread(c, DIMS[c][2], line(w, p, c), THIRD[i])

    for j, by in enumerate((1, 3)):
        for c in colors:
            p = source(DIMS[c][1], by)
            arrived(line(w, p, c), gather_sem.at[c, SECOND + j])
            onward(c, DIMS[c][1], p, by, SECOND)
    for i in (1, 2):
        for c in colors:
            third(c, i)
            relay(line(w, source(DIMS[c][1], BY[i]), c))

    def third_near(i):
        for j, by in enumerate((1, 3)):
            for c in colors:
                p = source(DIMS[c][2], by, source(DIMS[c][1], BY[i]))
                arrived(line(w, p, c), gather_sem.at[c, THIRD[i] + j])
                onward(c, DIMS[c][2], p, by, THIRD[i])
                relay(line(w, p, c))

    def third_far(i):
        for c in colors:
            p = source(DIMS[c][2], 2, source(DIMS[c][1], BY[i]))
            for half in (0, 1):
                arrived(line(w, p, c, half), gather_sem.at[c, THIRD[i] + 2 + half])
            relay(line(w, p, c))

    third_near(0)
    for c in colors:
        p = source(DIMS[c][1], 2)
        for half in (0, 1):
            arrived(line(w, p, c, half), gather_sem.at[c, SECOND + 2 + half])
        third(c, 3)
        relay(line(w, p, c))
    third_near(1)
    third_far(0)
    third_near(2)
    third_far(1)
    third_near(3)
    third_far(2)
    third_far(3)

    theirs = w.at[:, partner["c"]]
    pltpu.make_async_remote_copy(
        src_ref=theirs, dst_ref=theirs, send_sem=relay_send_sem, recv_sem=relay_sem,
        device_id=device(partner), device_id_type=MESH).wait()
    ours = w.at[:, me["c"]]
    drained = [ours.at[0], ours.at[1, pl.ds(0, 3)], ours.at[1, 3, 0], ours.at[1, 3, 1, pl.ds(0, 3)]]
    for part in drained:
        pltpu.make_async_remote_copy(
            src_ref=part, dst_ref=part, send_sem=send_sem, recv_sem=relay_sem,
            device_id=device(partner), device_id_type=MESH).wait_send()

    @pl.loop(1, WORKERS)
    def _(k):
        exchange(k).wait_send()
        var_exchange(k).wait_send()


def put_out(w, new_master, new_momentum, error, w_out, new_master_out, new_momentum_out, error_out, sem):
    pairs = ((w, w_out), (new_master, new_master_out), (new_momentum, new_momentum_out), (error, error_out))
    copies = []
    for i in range(8):
        rows = pl.ds(i * 256, 256)
        copies.append(pltpu.make_async_copy(w.at[rows], w_out.at[rows], sem.at[i]))
    for i, (a, b) in enumerate(pairs[1:]):
        copies.append(pltpu.make_async_copy(a, b, sem.at[8 + i]))
    for copy in copies:
        copy.start()
    for copy in copies:
        copy.wait()


def shards(grads, momentum, variance, master):
    f32 = jnp.float32
    vmem = pl.BlockSpec(memory_space=pltpu.VMEM)
    w, new_master, new_momentum, error = pl.pallas_call(
        step_kernel,
        out_shape=(
            pltpu.VMEM((2, 2, 4, 2, 4, ROWS, WIDTH), jnp.bfloat16),
            pltpu.VMEM((ROWS, WIDTH), f32),
            pltpu.VMEM((ROWS, WIDTH), f32),
            pltpu.VMEM((BLOCKS, WIDTH), f32),
        ),
        in_specs=[vmem] * 4,
        out_specs=(vmem,) * 4,
        scratch_shapes=[
            pltpu.VMEM((WORKERS, ROWS, WIDTH), jnp.bfloat16),
            pltpu.VMEM((WORKERS, ROWS, WIDTH), jnp.bfloat16),
            pltpu.VMEM((WORKERS, ROWS, PIECE), jnp.bfloat16),
            pltpu.VMEM((WORKERS, ROWS, PIECE), jnp.bfloat16),
            pltpu.SemaphoreType.DMA,
            pltpu.SemaphoreType.DMA((WORKERS,)),
            pltpu.SemaphoreType.DMA((WORKERS,)),
            pltpu.SemaphoreType.DMA((3, 23)),
            pltpu.SemaphoreType.DMA,
            pltpu.SemaphoreType.DMA,
            pltpu.SemaphoreType.DMA((WORKERS,)),
            pltpu.SemaphoreType.DMA((WORKERS,)),
        ],
        compiler_params=pltpu.CompilerParams(collective_id=0, has_side_effects=True, vmem_limit_bytes=36 << 20),
        name="step",
    )(grads, momentum, variance.T, master)
    w = w.reshape(BLOCKS * ROWS, WIDTH)
    anywhere = pl.BlockSpec(memory_space=pl.ANY)
    hbm = pl.BlockSpec(memory_space=pltpu.HBM)
    weights, new_master, new_momentum, error = pl.pallas_call(
        put_out,
        out_shape=(
            jax.ShapeDtypeStruct((BLOCKS * ROWS, WIDTH), jnp.bfloat16),
            jax.ShapeDtypeStruct((ROWS, WIDTH), f32),
            jax.ShapeDtypeStruct((ROWS, WIDTH), f32),
            jax.ShapeDtypeStruct((BLOCKS, WIDTH), f32),
        ),
        in_specs=[vmem] * 4,
        out_specs=(hbm,) * 4,
        scratch_shapes=[pltpu.SemaphoreType.DMA((11,))],
        compiler_params=pltpu.CompilerParams(vmem_limit_bytes=1 << 20),
        name="put_out",
    )(w, new_master, new_momentum, error)
    return weights, new_master, new_momentum, error[None]


def solution(mesh):
    return jax.shard_map(
        shards,
        mesh=mesh,
        in_specs=(
            P("gz", ("gx", "gy"), None),
            P(("gx", "gy"), None),
            P(("gx", "gy"), "gz"),
            P(("gx", "gy", "gz"), None),
        ),
        out_specs=(
            P(),
            P(("gx", "gy", "gz"), None),
            P(("gx", "gy", "gz"), None),
            P("gz", ("gx", "gy"), None),
        ),
        check_vma=False,
    )
```

```python
import jax
import jax.numpy as jnp
from jax import lax
from jax.experimental import pallas as pl
from jax.experimental.pallas import tpu as pltpu
from jax.sharding import PartitionSpec as P

beta_one = 0.9
learning_rate = 0.25
epsilon = 1e-08

MESH = pl.DeviceIdType.MESH
WORKERS = 8
ROWS = 16
WIDTH = 3584
PIECE = WIDTH // WORKERS
OTHERS = WORKERS - 1
BLOCKS = 128

DIMS = (("z", "x", "y"), ("x", "y", "z"), ("y", "z", "x"))
COLUMNS = ((0, 1280), (1280, 1152), (2432, 1152))
LONG = ()
ORDER = (
    ("e", 0), ("e", 2), ("e", 1), ("own", 0), ("p1", 0), ("own", 2), ("p1", 2), ("s0", 0), ("s0", 2), ("su", 0, 3),
    ("t00", 0), ("tu", 0, 3), ("own", 1), ("p1", 1), ("su", 0, 1), ("tu", 0, 1), ("s0", 1), ("tu", 0, 2),
    ("su", 0, 2), ("su", 2, 1), ("su", 2, 3), ("tu", 2, 2), ("su", 2, 2), ("t00", 2), ("tu", 2, 1), ("t00", 1),
    ("su", 1, 1), ("tu", 2, 3), ("su", 1, 3), ("su", 1, 2), ("tu", 1, 1), ("t", 0, 1, 1), ("r", 0, "t0", 1, 1),
    ("r", 0, "t0", 3, 0), ("tu", 1, 2), ("tu", 1, 3), ("sf", 2, 1), ("sf", 0, 3), ("sf", 0, 1), ("t", 2, 1, 1),
    ("sf", 2, 3), ("t", 0, 2, 1), ("t", 2, 2, 0), ("t", 1, 2, 0), ("tf", 2, 0, 3), ("sf", 1, 1), ("t", 1, 1, 0),
    ("sf", 1, 3), ("t", 0, 2, 0), ("t", 0, 1, 0), ("t", 2, 2, 1), ("t", 1, 1, 1), ("tf", 2, 0, 1), ("t", 0, 3, 0),
    ("r", 2, "t0", 1, 1), ("r", 2, "t0", 3, 0), ("r", 1, "t0", 1, 1), ("r", 1, "t0", 3, 0), ("r", 0, "t1", 1, 1),
    ("tf", 0, 2, 3), ("t", 1, 2, 1), ("t", 1, 3, 1), ("r", 0, "t2", 1, 1), ("r", 2, "t1", 1, 1), ("t", 0, 3, 1),
    ("t", 2, 1, 0), ("t", 1, 3, 0), ("r", 1, "t2", 3, 0), ("tf", 1, 1, 1), ("r", 2, "t2", 3, 0), ("t", 2, 3, 0),
    ("t", 2, 3, 1), ("tf", 1, 1, 3), ("r", 1, "t1", 3, 0), ("r", 0, "t2", 3, 0), ("r", 2, "t0", "far", 1),
    ("r", 2, "t2", 1, 1), ("tf", 1, 0, 3), ("tf", 0, 2, 1), ("tf", 2, 2, 3), ("r", 1, "t1", 1, 1), ("tf", 2, 1, 1),
    ("r", 2, "t0", "far", 0), ("r", 0, "t1", 3, 0), ("r", 1, "t2", 1, 1), ("tf", 0, 0, 3), ("tf", 2, 2, 1),
    ("tf", 1, 2, 1), ("tf", 2, 1, 3), ("tf", 0, 0, 1), ("tf", 1, 3, 3), ("r", 2, "t1", 3, 0), ("r", 0, "t3", 3, 0),
    ("tf", 1, 0, 1), ("tf", 0, 3, 1), ("tf", 0, 1, 3), ("tf", 2, 3, 3), ("r", 1, "t3", 1, 1), ("r", 2, "t3", 3, 0),
    ("r", 0, "t3", 1, 1), ("r", 0, "t2", "far", 1), ("r", 1, "t3", 3, 0), ("tf", 1, 3, 1), ("tf", 0, 3, 3),
    ("r", 2, "t3", 1, 1), ("tf", 2, 3, 1), ("tf", 1, 2, 3), ("tf", 0, 1, 1), ("r", 0, "t2", "far", 0),
    ("r", 1, "t1", "far", 1), ("r", 1, "t1", "far", 0), ("r", 2, "t2", "far", 1), ("r", 2, "t1", "far", 0),
    ("r", 0, "t0", "far", 0), ("r", 0, "t0", "far", 1), ("r", 1, "t0", "far", 1), ("r", 1, "t2", "far", 0),
    ("r", 2, "t1", "far", 1), ("r", 2, "t2", "far", 0), ("r", 0, "t3", "far", 0), ("r", 0, "t1", "far", 1),
    ("r", 1, "t3", "far", 1), ("r", 1, "t0", "far", 0), ("r", 2, "t3", "far", 1), ("r", 2, "t3", "far", 0),
    ("r", 1, "t2", "far", 1), ("r", 1, "t3", "far", 0), ("r", 0, "t1", "far", 0), ("r", 0, "t3", "far", 1),
)
LINES = ("s", "t0", "t1", "t2", "t3")


def device(p):
    return ((p["z"] // 2) * 2 + p["c"], p["y"], (p["z"] % 2) * 4 + p["x"])


def far(p, dim):
    return {**p, dim: lax.rem(p[dim] + 2, 4)}


def step(p, dim, dr):
    if dim != "z":
        return {**p, dim: lax.rem(p[dim] + dr, 4)}
    low = lax.rem(p["z"], 2)
    return {**p, dim: lax.rem(p["z"] + (5 - 2 * low if dr == 1 else 3 + 2 * low), 4)}


def back(p, dim, dr):
    return step(p, dim, 4 - dr) if dim != "z" else step(p, dim, dr)


def cols(c):
    return pl.ds(*COLUMNS[c])


def line(w, p, c, half):
    first = DIMS[c][0]
    zh, zl = p["z"] // 2, lax.rem(p["z"], 2)
    part = pl.ds(half * 2, 2)
    if first == "x":
        return w.at[zh, p["c"], p["y"], zl, part, :, cols(c)]
    if first == "y":
        return w.at[zh, p["c"], part, zl, p["x"], :, cols(c)]
    return w.at[half, p["c"], p["y"], :, p["x"], :, cols(c)]


def unit(w, p, c):
    return w.at[p["z"] // 2, p["c"], p["y"], lax.rem(p["z"], 2), p["x"], :, cols(c)]


def step_kernel(
    g_hbm, m_hbm, v_hbm, master_hbm,
    w, new_master_ref, new_momentum_ref, error_ref,
    g_ref, m_ref, v_ref, master_ref, sent, received, var_sent, var_received, scale,
    load_sem, exchange_sem, exchange_send_sem, var_sem, gather_sem, send_sem, relay_sem, relay_send_sem,
):
    gx, gy, gz = lax.axis_index("gx"), lax.axis_index("gy"), lax.axis_index("gz")
    me = {"x": lax.rem(gz, 4), "y": gy, "z": (gx // 2) * 2 + gz // 4, "c": lax.rem(gx, 2)}
    partner = {**me, "c": 1 - me["c"]}

    barrier = pltpu.get_barrier_semaphore()
    greeted = [(gx, gy, lax.rem(gz + k, WORKERS)) for k in range(1, WORKERS)]
    greeted += [device({**me, "y": lax.rem(gy + k, 4)}) for k in (1, 2, 3)]
    greeted += [device(step(me, "z", 3)), device(far(me, "z")), device(partner)]
    for d in greeted:
        pl.semaphore_signal(barrier, inc=1, device_id=d, device_id_type=MESH)

    def rows_of(owner):
        return pl.ds(pl.multiple_of(owner * ROWS, ROWS), ROWS)

    def loads(k):
        rows = rows_of(lax.rem(gz + k + 1, WORKERS))
        return (
            pltpu.make_async_copy(g_hbm.at[0, rows, :], g_ref.at[rows, :], load_sem.at[0, k]),
            pltpu.make_async_copy(m_hbm.at[rows, :], m_ref.at[rows, :], load_sem.at[1, k]),
        )

    load_var = pltpu.make_async_copy(v_hbm, v_ref, load_sem.at[2, 0])
    load_master = pltpu.make_async_copy(master_hbm, master_ref, load_sem.at[2, 1])
    load_var.start()

    @pl.loop(0, WORKERS)
    def _(k):
        for copy in loads(k):
            copy.start()

    load_master.start()

    load_var.wait()
    var = v_ref[...].T.astype(jnp.bfloat16)
    for k in range(WORKERS):
        var_sent[k] = var[k * ROWS:(k + 1) * ROWS, :]

    @pl.loop(0, WORKERS)
    def _(k):
        for copy in loads(k):
            copy.wait()
        owner = lax.rem(gz + k + 1, WORKERS)
        rows = rows_of(owner)
        corrected = beta_one * m_ref[rows, :] + (1.0 - beta_one) * g_ref[rows, :].astype(jnp.float32)
        level = jnp.mean(jnp.abs(corrected), axis=-1, keepdims=True).astype(jnp.bfloat16).astype(jnp.float32)
        compressed = jnp.where(corrected >= 0.0, level, -level)
        sent[owner] = compressed.astype(jnp.bfloat16)
        error_ref[rows, :] = corrected - compressed

    pl.semaphore_wait(barrier, len(greeted))

    def to_owner(k, src, dst, sems):
        owner = lax.rem(gz + k, WORKERS)
        pltpu.make_async_remote_copy(
            src_ref=src.at[owner, :, sems[2]], dst_ref=dst.at[gz, :, sems[2]], send_sem=sems[0], recv_sem=sems[1],
            device_id=(gx, gy, owner), device_id_type=MESH).start()

    def of_all(ref, sems):
        return pltpu.make_async_remote_copy(
            src_ref=ref.at[pl.ds(0, OTHERS), :, sems[2]], dst_ref=ref.at[pl.ds(0, OTHERS), :, sems[2]],
            send_sem=sems[0], recv_sem=sems[1], device_id=device(partner), device_id_type=MESH)

    var_sems = (var_sem.at[0], var_sem.at[1], slice(None))
    for k in range(1, WORKERS):
        to_owner(k, var_sent, var_received, var_sems)

    def exchange_sems(c):
        return (exchange_send_sem.at[c], exchange_sem.at[c], cols(c))

    def sem_of(nm, c, dr, half=None):
        if nm == "p1":
            return gather_sem.at[c, dr - 1]
        at = 3 + 6 * LINES.index(nm)
        return gather_sem.at[c, at + ((4 if dr == "far" else dr - 1) + half)]

    def send(src, to, sem):
        pltpu.make_async_remote_copy(
            src_ref=src, dst_ref=src, send_sem=send_sem, recv_sem=sem, device_id=device(to), device_id_type=MESH).start()

    def relay(src):
        pltpu.make_async_remote_copy(
            src_ref=src, dst_ref=src, send_sem=relay_send_sem, recv_sem=relay_sem,
            device_id=device(partner), device_id_type=MESH).start()

    def came_from(nm, c, dr):
        first, second, third = DIMS[c]
        if nm == "p1":
            return far(me, first) if dr == 2 else back(me, first, dr)
        if nm == "s":
            return far(me, second) if dr == "far" else back(me, second, dr)
        i = int(nm[1])
        p = (me, back(me, second, 1), back(me, second, 3), far(me, second))[i]
        return far(p, third) if dr == "far" else back(p, third, dr)

    def contents(nm, c, dr, half=None):
        p = came_from(nm, c, dr)
        return unit(w, p, c) if nm == "p1" else line(w, p, c, half)

    done = set()
    fresh = []

    def wait(nm, c, dr, half=None):
        if (nm, c, dr, half) in done:
            return
        done.add((nm, c, dr, half))
        held = contents(nm, c, dr, half)
        pltpu.make_async_remote_copy(
            src_ref=held, dst_ref=held, send_sem=send_sem, recv_sem=sem_of(nm, c, dr, half),
            device_id=device(partner), device_id_type=MESH).wait_recv()
        fresh.append(held)

    def send_unit(c, p, nm):
        dim = DIMS[c][1 if nm == "s" else 2]
        half = p[DIMS[c][0]] // 2
        for dr in (1, 3):
            send(unit(w, p, c), step(me, dim, dr), sem_of(nm, c, dr, half))

    def send_onward(c, dim, nm, dr):
        if dim == "z" and (nm, c) in LONG:
            halves = (0, 1) if dr == 1 else ()
        else:
            halves = (0,) if dr == 1 else (1,)
        for half in halves:
            wait(nm, c, dr, half)
        for half in halves:
            send(contents(nm, c, dr, half), step(me, dim, 4 - dr if dim == "z" else dr), sem_of(nm, c, "far", half))

    def update_scale():
        received[gz] = sent[gz]
        var_received[gz] = var_sent[gz]
        of_all(var_received, var_sems).wait_recv()
        for pair in range(WORKERS // 2):
            owned = jnp.concatenate(
                [var_received[2 * pair].astype(jnp.float32), var_received[2 * pair + 1].astype(jnp.float32)], axis=-1)
            scale[:, pl.ds(pair * 2 * PIECE, 2 * PIECE)] = jnp.sqrt(owned) + epsilon
        load_master.wait()

    def update(c):
        of_all(received, exchange_sems(c)).wait_recv()
        total = received[0, :, cols(c)].astype(jnp.float32)
        for k in range(1, WORKERS):
            total = total + received[k, :, cols(c)].astype(jnp.float32)
        new_momentum = total / WORKERS
        new_master = master_ref[:, cols(c)] - learning_rate * new_momentum / scale[:, cols(c)]
        w[me["z"] // 2, me["c"], me["y"], lax.rem(me["z"], 2), me["x"], :, cols(c)] = new_master.astype(jnp.bfloat16)
        new_momentum_ref[:, cols(c)] = new_momentum
        new_master_ref[:, cols(c)] = new_master

    updated = []
    for task in ORDER:
        kind, c = task[0], task[1]
        first, second, third = DIMS[c]
        if kind == "e":
            for k in range(1, WORKERS):
                to_owner(k, sent, received, exchange_sems(c))
        elif kind == "own":
            if not updated:
                update_scale()
            updated.append(c)
            update(c)
            fresh.append(unit(w, me, c))
        elif kind == "p1":
            for dr in (1, 3):
                send(unit(w, me, c), step(me, first, dr), sem_of("p1", c, dr))
            send(unit(w, me, c), far(me, first), sem_of("p1", c, 2))
        elif kind in ("s0", "t00"):
            send_unit(c, me, kind[:-1])
        elif kind in ("su", "tu"):
            wait("p1", c, task[2])
            send_unit(c, came_from("p1", c, task[2]), "s" if kind == "su" else "t0")
        elif kind == "sf":
            send_onward(c, second, "s", task[2])
        elif kind == "t":
            i, half = task[2:]
            dr = (1, 3, "far")[i - 1]
            wait("s", c, dr, half)
            for way in (1, 3):
                send(contents("s", c, dr, half), step(me, third, way), sem_of("t%d" % i, c, way, half))
        elif kind == "tf":
            send_onward(c, third, "t%d" % task[2], task[3])
        else:
            wait(task[2], c, *task[3:])
        if kind not in ("own", "p1", "s0"):
            for held in fresh:
                relay(held)
            fresh.clear()

    theirs = w.at[:, partner["c"]]
    pltpu.make_async_remote_copy(
        src_ref=theirs, dst_ref=theirs, send_sem=relay_send_sem, recv_sem=relay_sem,
        device_id=device(partner), device_id_type=MESH).wait()
    ours = w.at[:, me["c"]]
    for part in (ours.at[0], ours.at[1, pl.ds(0, 3)], ours.at[1, 3, 0], ours.at[1, 3, 1, pl.ds(0, 3)]):
        pltpu.make_async_remote_copy(
            src_ref=part, dst_ref=part, send_sem=send_sem, recv_sem=relay_sem,
            device_id=device(partner), device_id_type=MESH).wait_send()
    of_all(var_sent, var_sems).wait_send()
    for c in range(3):
        of_all(sent, exchange_sems(c)).wait_send()


def put_out(w, new_master, new_momentum, error, w_out, new_master_out, new_momentum_out, error_out, sem):
    copies = []
    for i in range(8):
        rows = pl.ds(i * 256, 256)
        copies.append(pltpu.make_async_copy(w.at[rows], w_out.at[rows], sem.at[i]))
    pairs = ((new_master, new_master_out), (new_momentum, new_momentum_out), (error, error_out))
    for i, (a, b) in enumerate(pairs):
        copies.append(pltpu.make_async_copy(a, b, sem.at[8 + i]))
    for copy in copies:
        copy.start()
    for copy in copies:
        copy.wait()


def shards(grads, momentum, variance, master):
    f32 = jnp.float32
    vmem = pl.BlockSpec(memory_space=pltpu.VMEM)
    hbm = pl.BlockSpec(memory_space=pltpu.HBM)
    w, new_master, new_momentum, error = pl.pallas_call(
        step_kernel,
        out_shape=(
            pltpu.VMEM((2, 2, 4, 2, 4, ROWS, WIDTH), jnp.bfloat16),
            pltpu.VMEM((ROWS, WIDTH), f32),
            pltpu.VMEM((ROWS, WIDTH), f32),
            pltpu.VMEM((BLOCKS, WIDTH), f32),
        ),
        in_specs=[hbm] * 4,
        out_specs=(vmem,) * 4,
        scratch_shapes=[
            pltpu.VMEM((BLOCKS, WIDTH), jnp.bfloat16),
            pltpu.VMEM((BLOCKS, WIDTH), f32),
            pltpu.VMEM((PIECE, BLOCKS), f32),
            pltpu.VMEM((ROWS, WIDTH), f32),
            pltpu.VMEM((WORKERS, ROWS, WIDTH), jnp.bfloat16),
            pltpu.VMEM((WORKERS, ROWS, WIDTH), jnp.bfloat16),
            pltpu.VMEM((WORKERS, ROWS, PIECE), jnp.bfloat16),
            pltpu.VMEM((WORKERS, ROWS, PIECE), jnp.bfloat16),
            pltpu.VMEM((ROWS, WIDTH), f32),
            pltpu.SemaphoreType.DMA((3, WORKERS)),
            pltpu.SemaphoreType.DMA((3,)),
            pltpu.SemaphoreType.DMA((3,)),
            pltpu.SemaphoreType.DMA((2,)),
            pltpu.SemaphoreType.DMA((3, 33)),
            pltpu.SemaphoreType.DMA,
            pltpu.SemaphoreType.DMA,
            pltpu.SemaphoreType.DMA,
        ],
        compiler_params=pltpu.CompilerParams(collective_id=0, has_side_effects=True, vmem_limit_bytes=36 << 20),
        name="step",
    )(grads, momentum, variance.T, master)
    w = w.reshape(BLOCKS * ROWS, WIDTH)
    weights, new_master, new_momentum, error = pl.pallas_call(
        put_out,
        out_shape=(
            jax.ShapeDtypeStruct((BLOCKS * ROWS, WIDTH), jnp.bfloat16),
            jax.ShapeDtypeStruct((ROWS, WIDTH), f32),
            jax.ShapeDtypeStruct((ROWS, WIDTH), f32),
            jax.ShapeDtypeStruct((BLOCKS, WIDTH), f32),
        ),
        in_specs=[vmem] * 4,
        out_specs=(hbm,) * 4,
        scratch_shapes=[pltpu.SemaphoreType.DMA((11,))],
        compiler_params=pltpu.CompilerParams(vmem_limit_bytes=1 << 20),
        name="put_out",
    )(w, new_master, new_momentum, error)
    return weights, new_master, new_momentum, error[None]


def solution(mesh):
    return jax.shard_map(
        shards,
        mesh=mesh,
        in_specs=(
            P("gz", ("gx", "gy"), None),
            P(("gx", "gy"), None),
            P(("gx", "gy"), "gz"),
            P(("gx", "gy", "gz"), None),
        ),
        out_specs=(
            P(),
            P(("gx", "gy", "gz"), None),
            P(("gx", "gy", "gz"), None),
            P("gz", ("gx", "gy"), None),
        ),
        check_vma=False,
    )
```

```python
import jax
import jax.numpy as jnp
from jax import lax
from jax.experimental import pallas as pl
from jax.experimental.pallas import tpu as pltpu
from jax.sharding import PartitionSpec as P

beta_one = 0.9
learning_rate = 0.25
epsilon = 1e-08

MESH = pl.DeviceIdType.MESH
WORKERS = 8
ROWS = 16
WIDTH = 3584
PIECE = WIDTH // WORKERS
OTHERS = WORKERS - 1
BLOCKS = 128

DIMS = (("y", "z", "x"), ("y", "z", "x"), ("x", "z", "y"), ("x", "y", "z"), ("x", "y", "z"), ("x", "z", "y"))
COLUMNS = ((0, 768), (768, 640), (1408, 640), (2048, 640), (2688, 384), (3072, 512))
COLORS = len(COLUMNS)
LONG = (("t2", 4),)
ORDER = (
    ("e", 0), ("e", 1), ("e", 2), ("e", 4), ("e", 5), ("e", 3), ("own", 0), ("p1", 0), ("own", 1), ("s0", 0),
    ("s0", 1), ("p1", 1), ("own", 2), ("s0", 2), ("p1", 2), ("su", 0, 3), ("own", 4), ("t00", 2), ("p1", 4),
    ("su", 0, 1), ("t00", 4), ("tu", 0, 3), ("tu", 0, 1), ("su", 0, 2), ("su", 1, 1), ("su", 1, 3), ("own", 5),
    ("p1", 5), ("t00", 1), ("s0", 5), ("su", 1, 2), ("own", 3), ("t00", 3), ("p1", 3), ("s0", 4), ("su", 2, 3),
    ("tu", 2, 1), ("su", 2, 1), ("tu", 1, 3), ("tu", 2, 3), ("su", 2, 2), ("su", 4, 1), ("t00", 0), ("tu", 1, 1),
    ("tu", 4, 3), ("tu", 2, 2), ("tu", 4, 1), ("su", 4, 2), ("su", 4, 3), ("sf", 0, 1), ("t00", 5), ("tu", 1, 2),
    ("su", 5, 3), ("tu", 5, 3), ("su", 5, 1), ("tu", 5, 1), ("tu", 4, 2), ("t", 0, 1, 1), ("s0", 3), ("tu", 0, 2),
    ("su", 5, 2), ("t", 0, 2, 0), ("t", 1, 1, 1), ("t", 1, 2, 1), ("sf", 1, 3), ("sf", 1, 1), ("t", 1, 1, 0),
    ("su", 3, 3), ("tu", 5, 2), ("su", 3, 1), ("tu", 3, 3), ("su", 3, 2), ("sf", 2, 3), ("t", 1, 2, 0),
    ("t", 2, 1, 1), ("sf", 2, 1), ("sf", 0, 3), ("sf", 4, 3), ("r", 2, "t0", 1, 1), ("r", 2, "t0", 3, 0),
    ("tu", 3, 2), ("sf", 4, 1), ("t", 4, 2, 1), ("t", 4, 1, 0), ("t", 4, 1, 1), ("t", 2, 1, 0), ("t", 2, 2, 0),
    ("tf", 1, 0, 1), ("tf", 0, 0, 1), ("r", 1, "t0", 1, 1), ("r", 1, "t0", 3, 0), ("r", 0, "t1", 1, 1),
    ("r", 4, "t0", 1, 1), ("t", 5, 1, 0), ("tf", 5, 0, 1), ("r", 4, "t0", 3, 0), ("r", 0, "t0", 1, 1), ("t", 0, 2, 1),
    ("r", 0, "t0", 3, 0), ("tf", 5, 0, 3), ("sf", 5, 1), ("t", 0, 1, 0), ("sf", 3, 1), ("r", 5, "t0", 1, 1),
    ("r", 5, "t0", 3, 0), ("tf", 4, 0, 3), ("t", 4, 2, 0), ("t", 1, 3, 1), ("t", 0, 3, 0), ("r", 0, "t2", 3, 0),
    ("t", 5, 1, 1), ("sf", 3, 3), ("t", 5, 2, 1), ("t", 3, 1, 1), ("tf", 4, 2, 3), ("t", 1, 3, 0), ("t", 5, 2, 0),
    ("tf", 1, 1, 3), ("t", 2, 3, 1), ("sf", 5, 3), ("t", 3, 2, 0), ("tf", 0, 1, 3), ("t", 3, 1, 0), ("t", 2, 3, 0),
    ("r", 1, "t1", 1, 1), ("t", 4, 3, 1), ("r", 2, "t1", 1, 1), ("t", 3, 2, 1), ("tu", 3, 1), ("tf", 0, 2, 1),
    ("tf", 2, 1, 1), ("r", 1, "t2", 1, 1), ("t", 4, 3, 0), ("tf", 4, 1, 1), ("r", 4, "t2", 3, 1),
    ("r", 2, "t1", 3, 0), ("r", 1, "t1", 3, 0), ("r", 4, "t1", 3, 0), ("t", 5, 3, 0), ("r", 2, "t2", 3, 0),
    ("r", 1, "t2", 3, 0), ("t", 3, 3, 0), ("r", 4, "t1", 1, 1), ("r", 5, "t1", 3, 0), ("r", 1, "t0", "far", 0),
    ("r", 4, "t0", "far", 1), ("r", 4, "t2", 3, 0), ("r", 5, "t0", "far", 0), ("r", 5, "t0", "far", 1),
    ("t", 3, 3, 1), ("r", 0, "t0", "far", 0), ("r", 0, "t1", 3, 0), ("r", 3, "t1", 1, 1), ("t", 0, 3, 1),
    ("tf", 5, 1, 1), ("t", 5, 3, 1), ("tf", 1, 3, 3), ("tf", 4, 2, 1), ("tf", 1, 2, 3), ("tf", 3, 1, 3),
    ("tf", 0, 2, 3), ("r", 5, "t1", 1, 1), ("t", 2, 2, 1), ("r", 3, "t2", 3, 0), ("r", 0, "t2", 1, 1),
    ("tf", 5, 2, 3), ("tf", 2, 3, 3), ("r", 5, "t2", 1, 1), ("r", 3, "t1", 3, 0), ("r", 0, "t3", 3, 0),
    ("r", 5, "t2", 3, 0), ("tf", 3, 1, 1), ("tf", 3, 2, 3), ("tf", 0, 1, 1), ("tf", 4, 1, 3), ("tf", 5, 2, 1),
    ("r", 1, "t3", 1, 1), ("tf", 2, 0, 3), ("r", 1, "t3", 3, 0), ("tf", 1, 2, 1), ("tf", 2, 3, 1),
    ("r", 2, "t3", 1, 1), ("r", 4, "t3", 1, 1), ("tf", 3, 0, 3), ("tf", 1, 0, 3), ("tf", 0, 0, 3),
    ("r", 3, "t0", 3, 0), ("tf", 3, 0, 1), ("r", 1, "t1", "far", 1), ("r", 2, "t3", 3, 0), ("r", 4, "t3", 3, 0),
    ("tf", 5, 1, 3), ("tf", 4, 3, 1), ("r", 3, "t2", 1, 1), ("r", 4, "t1", "far", 0), ("r", 3, "t0", 1, 1),
    ("r", 5, "t3", 3, 0), ("tf", 0, 3, 1), ("tf", 2, 0, 1), ("r", 0, "t1", "far", 1), ("tf", 2, 2, 1),
    ("tf", 5, 3, 3), ("r", 2, "t1", "far", 0), ("tf", 5, 3, 1), ("tf", 3, 2, 1), ("tf", 4, 0, 1), ("tf", 1, 1, 1),
    ("tf", 3, 3, 1), ("r", 3, "t3", 3, 0), ("tf", 3, 3, 3), ("r", 0, "t2", "far", 0), ("tf", 4, 3, 3),
    ("tf", 0, 3, 3), ("tf", 2, 1, 3), ("tf", 2, 2, 3), ("tf", 1, 3, 1), ("r", 5, "t1", "far", 0),
    ("r", 1, "t3", "far", 1), ("r", 0, "t3", 1, 1), ("r", 4, "t2", "far", 0), ("r", 3, "t3", 1, 1),
    ("r", 5, "t3", 1, 1), ("r", 5, "t2", "far", 1), ("r", 4, "t2", "far", 1), ("r", 1, "t2", "far", 1),
    ("r", 3, "t1", "far", 1), ("r", 2, "t2", 1, 1), ("r", 2, "t3", "far", 1), ("r", 0, "t1", "far", 0),
    ("r", 3, "t1", "far", 0), ("r", 5, "t2", "far", 0), ("r", 0, "t2", "far", 1), ("r", 3, "t2", "far", 1),
    ("r", 2, "t0", "far", 1), ("r", 1, "t2", "far", 0), ("r", 3, "t0", "far", 0), ("r", 4, "t1", "far", 1),
    ("r", 2, "t3", "far", 0), ("r", 5, "t1", "far", 1), ("r", 1, "t0", "far", 1), ("r", 4, "t3", "far", 0),
    ("r", 0, "t3", "far", 0), ("r", 3, "t0", "far", 1), ("r", 5, "t3", "far", 1), ("r", 2, "t0", "far", 0),
    ("r", 0, "t0", "far", 1), ("r", 3, "t2", "far", 0), ("r", 1, "t1", "far", 0), ("r", 3, "t3", "far", 1),
    ("r", 2, "t1", "far", 1), ("r", 4, "t0", "far", 0), ("r", 2, "t2", "far", 0), ("r", 4, "t3", "far", 1),
    ("r", 1, "t3", "far", 0), ("r", 0, "t3", "far", 1), ("r", 5, "t3", "far", 0), ("r", 2, "t2", "far", 1),
    ("r", 3, "t3", "far", 0),
)
LINES = ("s", "t0", "t1", "t2", "t3")


def device(p):
    return ((p["z"] // 2) * 2 + p["c"], p["y"], (p["z"] % 2) * 4 + p["x"])


def far(p, dim):
    return {**p, dim: lax.rem(p[dim] + 2, 4)}


def step(p, dim, dr):
    if dim != "z":
        return {**p, dim: lax.rem(p[dim] + dr, 4)}
    low = lax.rem(p["z"], 2)
    return {**p, dim: lax.rem(p["z"] + (5 - 2 * low if dr == 1 else 3 + 2 * low), 4)}


def back(p, dim, dr):
    return step(p, dim, 4 - dr) if dim != "z" else step(p, dim, dr)


def cols(c):
    return pl.ds(*COLUMNS[c])


def line(w, p, c, half):
    first = DIMS[c][0]
    zh, zl = p["z"] // 2, lax.rem(p["z"], 2)
    part = pl.ds(half * 2, 2)
    if first == "x":
        return w.at[zh, p["c"], p["y"], zl, part, :, cols(c)]
    if first == "y":
        return w.at[zh, p["c"], part, zl, p["x"], :, cols(c)]
    return w.at[half, p["c"], p["y"], :, p["x"], :, cols(c)]


def unit(w, p, c):
    return w.at[p["z"] // 2, p["c"], p["y"], lax.rem(p["z"], 2), p["x"], :, cols(c)]


def step_kernel(
    g_hbm, m_hbm, v_hbm, master_hbm,
    w, new_master_ref, new_momentum_ref, error_ref,
    g_ref, m_ref, v_ref, master_ref, sent, received, var_sent, var_received, scale,
    load_sem, exchange_sem, exchange_send_sem, var_sem, gather_sem, send_sem, relay_sem, relay_send_sem,
):
    gx, gy, gz = lax.axis_index("gx"), lax.axis_index("gy"), lax.axis_index("gz")
    me = {"x": lax.rem(gz, 4), "y": gy, "z": (gx // 2) * 2 + gz // 4, "c": lax.rem(gx, 2)}
    partner = {**me, "c": 1 - me["c"]}

    barrier = pltpu.get_barrier_semaphore()
    greeted = [(gx, gy, lax.rem(gz + k, WORKERS)) for k in range(1, WORKERS)]
    greeted += [device({**me, "y": lax.rem(gy + k, 4)}) for k in (1, 2, 3)]
    greeted += [device(step(me, "z", 3)), device(far(me, "z")), device(partner)]
    for d in greeted:
        pl.semaphore_signal(barrier, inc=1, device_id=d, device_id_type=MESH)

    def rows_of(owner):
        return pl.ds(pl.multiple_of(owner * ROWS, ROWS), ROWS)

    def loads(k):
        rows = rows_of(lax.rem(gz + k + 1, WORKERS))
        return (
            pltpu.make_async_copy(g_hbm.at[0, rows, :], g_ref.at[rows, :], load_sem.at[0, k]),
            pltpu.make_async_copy(m_hbm.at[rows, :], m_ref.at[rows, :], load_sem.at[1, k]),
        )

    load_var = pltpu.make_async_copy(v_hbm, v_ref, load_sem.at[2, 0])
    load_master = pltpu.make_async_copy(master_hbm, master_ref, load_sem.at[2, 1])
    load_var.start()

    @pl.loop(0, WORKERS)
    def _(k):
        for copy in loads(k):
            copy.start()

    load_master.start()

    load_var.wait()
    var = v_ref[...].T.astype(jnp.bfloat16)
    for k in range(WORKERS):
        var_sent[k] = var[k * ROWS:(k + 1) * ROWS, :]

    pl.semaphore_wait(barrier, len(greeted))

    def to_owner(k, src, dst, sems):
        owner = lax.rem(gz + k, WORKERS)
        pltpu.make_async_remote_copy(
            src_ref=src.at[owner, :, sems[2]], dst_ref=dst.at[gz, :, sems[2]], send_sem=sems[0], recv_sem=sems[1],
            device_id=(gx, gy, owner), device_id_type=MESH).start()

    def of_all(ref, sems):
        return pltpu.make_async_remote_copy(
            src_ref=ref.at[pl.ds(0, OTHERS), :, sems[2]], dst_ref=ref.at[pl.ds(0, OTHERS), :, sems[2]],
            send_sem=sems[0], recv_sem=sems[1], device_id=device(partner), device_id_type=MESH)

    var_sems = (var_sem.at[0], var_sem.at[1], slice(None))
    for k in range(1, WORKERS):
        to_owner(k, var_sent, var_received, var_sems)

    def exchange_sems(c):
        return (exchange_send_sem.at[c], exchange_sem.at[c], cols(c))

    def compress(k):
        for copy in loads(k):
            copy.wait()
        owner = lax.rem(gz + k + 1, WORKERS)
        rows = rows_of(owner)
        corrected = beta_one * m_ref[rows, :] + (1.0 - beta_one) * g_ref[rows, :].astype(jnp.float32)
        level = jnp.mean(jnp.abs(corrected), axis=-1, keepdims=True).astype(jnp.bfloat16).astype(jnp.float32)
        compressed = jnp.where(corrected >= 0.0, level, -level)
        sent[owner] = compressed.astype(jnp.bfloat16)
        error_ref[rows, :] = corrected - compressed

    compress(0)

    @pl.loop(1, WORKERS)
    def _(k):
        compress(k)
        to_owner(k, sent, received, exchange_sems(ORDER[0][1]))

    def sem_of(nm, c, dr, half=None):
        if nm == "p1":
            return gather_sem.at[c, dr - 1]
        at = 3 + 6 * LINES.index(nm)
        return gather_sem.at[c, at + ((4 if dr == "far" else dr - 1) + half)]

    def send(src, to, sem):
        pltpu.make_async_remote_copy(
            src_ref=src, dst_ref=src, send_sem=send_sem, recv_sem=sem, device_id=device(to), device_id_type=MESH).start()

    def relay(src):
        pltpu.make_async_remote_copy(
            src_ref=src, dst_ref=src, send_sem=relay_send_sem, recv_sem=relay_sem,
            device_id=device(partner), device_id_type=MESH).start()

    def came_from(nm, c, dr):
        first, second, third = DIMS[c]
        if nm == "p1":
            return far(me, first) if dr == 2 else back(me, first, dr)
        if nm == "s":
            return far(me, second) if dr == "far" else back(me, second, dr)
        i = int(nm[1])
        p = (me, back(me, second, 1), back(me, second, 3), far(me, second))[i]
        return far(p, third) if dr == "far" else back(p, third, dr)

    def contents(nm, c, dr, half=None):
        p = came_from(nm, c, dr)
        return unit(w, p, c) if nm == "p1" else line(w, p, c, half)

    done = set()
    fresh = []

    def wait(nm, c, dr, half=None):
        if (nm, c, dr, half) in done:
            return
        done.add((nm, c, dr, half))
        held = contents(nm, c, dr, half)
        pltpu.make_async_remote_copy(
            src_ref=held, dst_ref=held, send_sem=send_sem, recv_sem=sem_of(nm, c, dr, half),
            device_id=device(partner), device_id_type=MESH).wait_recv()
        fresh.append(held)

    def send_unit(c, p, nm):
        dim = DIMS[c][1 if nm == "s" else 2]
        half = p[DIMS[c][0]] // 2
        for dr in (1, 3):
            send(unit(w, p, c), step(me, dim, dr), sem_of(nm, c, dr, half))

    def send_onward(c, dim, nm, dr):
        if dim == "z" and (nm, c) in LONG:
            halves = (0, 1) if dr == 1 else ()
        else:
            halves = (0,) if dr == 1 else (1,)
        for half in halves:
            wait(nm, c, dr, half)
        for half in halves:
            send(contents(nm, c, dr, half), step(me, dim, 4 - dr if dim == "z" else dr), sem_of(nm, c, "far", half))

    def update_scale():
        received[gz] = sent[gz]
        var_received[gz] = var_sent[gz]
        of_all(var_received, var_sems).wait_recv()
        for pair in range(WORKERS // 2):
            owned = jnp.concatenate(
                [var_received[2 * pair].astype(jnp.float32), var_received[2 * pair + 1].astype(jnp.float32)], axis=-1)
            scale[:, pl.ds(pair * 2 * PIECE, 2 * PIECE)] = jnp.sqrt(owned) + epsilon
        load_master.wait()

    def update(c):
        of_all(received, exchange_sems(c)).wait_recv()
        total = received[0, :, cols(c)].astype(jnp.float32)
        for k in range(1, WORKERS):
            total = total + received[k, :, cols(c)].astype(jnp.float32)
        new_momentum = total / WORKERS
        new_master = master_ref[:, cols(c)] - learning_rate * new_momentum / scale[:, cols(c)]
        w[me["z"] // 2, me["c"], me["y"], lax.rem(me["z"], 2), me["x"], :, cols(c)] = new_master.astype(jnp.bfloat16)
        new_momentum_ref[:, cols(c)] = new_momentum
        new_master_ref[:, cols(c)] = new_master

    updated = []
    for task in ORDER[1:]:
        kind, c = task[0], task[1]
        first, second, third = DIMS[c]
        if kind == "e":
            for k in range(1, WORKERS):
                to_owner(k, sent, received, exchange_sems(c))
        elif kind == "own":
            if not updated:
                update_scale()
            updated.append(c)
            update(c)
            fresh.append(unit(w, me, c))
        elif kind == "p1":
            for dr in (1, 3):
                send(unit(w, me, c), step(me, first, dr), sem_of("p1", c, dr))
            send(unit(w, me, c), far(me, first), sem_of("p1", c, 2))
        elif kind in ("s0", "t00"):
            send_unit(c, me, kind[:-1])
        elif kind in ("su", "tu"):
            wait("p1", c, task[2])
            send_unit(c, came_from("p1", c, task[2]), "s" if kind == "su" else "t0")
        elif kind == "sf":
            send_onward(c, second, "s", task[2])
        elif kind == "t":
            i, half = task[2:]
            dr = (1, 3, "far")[i - 1]
            wait("s", c, dr, half)
            for way in (1, 3):
                send(contents("s", c, dr, half), step(me, third, way), sem_of("t%d" % i, c, way, half))
        elif kind == "tf":
            send_onward(c, third, "t%d" % task[2], task[3])
        else:
            wait(task[2], c, *task[3:])
        if kind not in ("own", "p1", "s0"):
            for held in fresh:
                relay(held)
            fresh.clear()

    theirs = w.at[:, partner["c"]]
    pltpu.make_async_remote_copy(
        src_ref=theirs, dst_ref=theirs, send_sem=relay_send_sem, recv_sem=relay_sem,
        device_id=device(partner), device_id_type=MESH).wait()
    ours = w.at[:, me["c"]]
    for part in (ours.at[0], ours.at[1, pl.ds(0, 3)], ours.at[1, 3, 0], ours.at[1, 3, 1, pl.ds(0, 3)]):
        pltpu.make_async_remote_copy(
            src_ref=part, dst_ref=part, send_sem=send_sem, recv_sem=relay_sem,
            device_id=device(partner), device_id_type=MESH).wait_send()
    of_all(var_sent, var_sems).wait_send()
    for c in range(COLORS):
        of_all(sent, exchange_sems(c)).wait_send()


def put_out(w, new_master, new_momentum, error, w_out, new_master_out, new_momentum_out, error_out, sem):
    copies = []
    for i in range(8):
        rows = pl.ds(i * 256, 256)
        copies.append(pltpu.make_async_copy(w.at[rows], w_out.at[rows], sem.at[i]))
    pairs = ((new_master, new_master_out), (new_momentum, new_momentum_out), (error, error_out))
    for i, (a, b) in enumerate(pairs):
        copies.append(pltpu.make_async_copy(a, b, sem.at[8 + i]))
    for copy in copies:
        copy.start()
    for copy in copies:
        copy.wait()


def shards(grads, momentum, variance, master):
    f32 = jnp.float32
    vmem = pl.BlockSpec(memory_space=pltpu.VMEM)
    hbm = pl.BlockSpec(memory_space=pltpu.HBM)
    w, new_master, new_momentum, error = pl.pallas_call(
        step_kernel,
        out_shape=(
            pltpu.VMEM((2, 2, 4, 2, 4, ROWS, WIDTH), jnp.bfloat16),
            pltpu.VMEM((ROWS, WIDTH), f32),
            pltpu.VMEM((ROWS, WIDTH), f32),
            pltpu.VMEM((BLOCKS, WIDTH), f32),
        ),
        in_specs=[hbm] * 4,
        out_specs=(vmem,) * 4,
        scratch_shapes=[
            pltpu.VMEM((BLOCKS, WIDTH), jnp.bfloat16),
            pltpu.VMEM((BLOCKS, WIDTH), f32),
            pltpu.VMEM((PIECE, BLOCKS), f32),
            pltpu.VMEM((ROWS, WIDTH), f32),
            pltpu.VMEM((WORKERS, ROWS, WIDTH), jnp.bfloat16),
            pltpu.VMEM((WORKERS, ROWS, WIDTH), jnp.bfloat16),
            pltpu.VMEM((WORKERS, ROWS, PIECE), jnp.bfloat16),
            pltpu.VMEM((WORKERS, ROWS, PIECE), jnp.bfloat16),
            pltpu.VMEM((ROWS, WIDTH), f32),
            pltpu.SemaphoreType.DMA((3, WORKERS)),
            pltpu.SemaphoreType.DMA((COLORS,)),
            pltpu.SemaphoreType.DMA((COLORS,)),
            pltpu.SemaphoreType.DMA((2,)),
            pltpu.SemaphoreType.DMA((COLORS, 33)),
            pltpu.SemaphoreType.DMA,
            pltpu.SemaphoreType.DMA,
            pltpu.SemaphoreType.DMA,
        ],
        compiler_params=pltpu.CompilerParams(collective_id=0, has_side_effects=True, vmem_limit_bytes=36 << 20),
        name="step",
    )(*(pltpu.with_memory_space_constraint(a, pltpu.HBM) for a in (grads, momentum, variance.T, master)))
    w = w.reshape(BLOCKS * ROWS, WIDTH)
    weights, new_master, new_momentum, error = pl.pallas_call(
        put_out,
        out_shape=(
            jax.ShapeDtypeStruct((BLOCKS * ROWS, WIDTH), jnp.bfloat16),
            jax.ShapeDtypeStruct((ROWS, WIDTH), f32),
            jax.ShapeDtypeStruct((ROWS, WIDTH), f32),
            jax.ShapeDtypeStruct((BLOCKS, WIDTH), f32),
        ),
        in_specs=[vmem] * 4,
        out_specs=(hbm,) * 4,
        scratch_shapes=[pltpu.SemaphoreType.DMA((11,))],
        compiler_params=pltpu.CompilerParams(vmem_limit_bytes=1 << 20),
        name="put_out",
    )(w, new_master, new_momentum, error)
    return weights, new_master, new_momentum, error[None]


def solution(mesh):
    return jax.shard_map(
        shards,
        mesh=mesh,
        in_specs=(
            P("gz", ("gx", "gy"), None),
            P(("gx", "gy"), None),
            P(("gx", "gy"), "gz"),
            P(("gx", "gy", "gz"), None),
        ),
        out_specs=(
            P(),
            P(("gx", "gy", "gz"), None),
            P(("gx", "gy", "gz"), None),
            P("gz", ("gx", "gy"), None),
        ),
        check_vma=False,
    )
```
